128 devices in a mesh: expert: 8 (over z, core), shard: 16 (over y, x).
Axes of the slice: x: 4, y: 4, z: 4, core: 2. Of those that a mesh axis runs over, the one named last changes fastest.
Arguments:
- master_down: float32 [16, 6400, 4096], P('expert', None, 'shard'), may hold values from -0.109375 to 0.109375
- second_down: bfloat16 [16, 6400, 4096], P('expert', None, 'shard'), may hold values from -0.0390625 to 0.0390625
- router_weight: float32 [4096, 16], P('shard', 'expert'), may hold values from -0.09375 to 0.09375
- router_gain: float32 [4096], P('shard'), may hold values from 0.25 to 1.75
Outputs:
- final_down: bfloat16 [16, 6400, 4096], P('expert', 'shard')
- scale_down: float32 [16, 6400], P('expert', 'shard')
- serve_router: bfloat16 [4096, 16], replicated
The draws below stay inside these ranges and needn't reach their ends.
All inputs are finite; a program needn't handle non-finite values.
Results may differ from the reference program's by a relative error of at most 0.001.
Values may be sent and summed in bfloat16 or wider, within the bound.
A program may use at most 128 MiB of HBM per device.

```python
import jax
import jax.numpy as jnp
from jax import lax

EXPERTS = 16
D_MODEL = 4096
D_EXPERT = 6400


def spiked(values, stream_key, source, target, blocks, factor):
    def block_of(position):
        return (jnp.arange(values.shape[position]) // (values.shape[position] // blocks)).reshape((-1,) + (1,) * (values.ndim - 1 - position))

    one_side = jax.random.permutation(stream_key, blocks)[block_of(target)]
    other_side = (block_of(target) + blocks // 2) % blocks
    return jnp.where((block_of(source) == one_side) | (block_of(source) == other_side), factor * values, values)


def level_of(key, shape, split, low, top_value):
    loudness, own = 1.0, jax.random.fold_in(key, 6)
    for position, parts in split:
        draws = jnp.exp(jax.random.uniform(jax.random.fold_in(own, position), (parts,), jnp.float32, low / len(split), top_value / len(split)))
        loudness = loudness * jnp.repeat(draws, shape[position] // parts).reshape([-1 if axis == position else 1 for axis in range(len(shape))])
    return loudness


def bell_draw(key, shape, width, most, shards=(), kind=jnp.bfloat16):
    entries = width * jax.random.normal(key, shape, jnp.float32)
    if shards:
        entries = entries * level_of(key, shape, shards, -0.22, 0.18)
    return jnp.clip(entries, -most, most).astype(kind)


def bell_draw_with(rng, shape, scale, most, split, heavy, dtype=jnp.bfloat16):
    array = scale * jax.random.normal(rng, shape, jnp.float32)
    if split:
        array = array * level_of(rng, shape, split, -0.22, 0.18)
    return jnp.clip(spiked(array, jax.random.fold_in(rng, 3), *heavy), -most, most).astype(dtype)


def setup_inputs(seed: int = 0) -> dict:
    splits = jax.random.split(jax.random.key(seed), 5)
    return {
        "master_down": bell_draw_with(splits[0], (EXPERTS, D_EXPERT, D_MODEL), D_EXPERT ** -0.5, 0.109375, ((0, 8), (2, 16)), (2, 1, 16, 2.0), jnp.float32),
        "second_down": bell_draw(splits[1], (EXPERTS, D_EXPERT, D_MODEL), (D_EXPERT * 4) ** -0.5, 0.0390625, ((0, 8), (2, 16))),
        "router_weight": bell_draw(splits[2], (D_MODEL, EXPERTS), D_MODEL ** -0.5, 0.09375, ((0, 16), (1, 8)), jnp.float32),
        "router_gain": jnp.clip(1.0 + 0.15 * jax.random.normal(splits[3], (D_MODEL,), jnp.float32), 0.25, 1.75),
    }


def reference(master_down, second_down, router_weight, router_gain):
    merged_down = master_down + second_down.astype(jnp.float32)
    scale_down = jnp.sqrt(lax.optimization_barrier(jnp.sum(merged_down * merged_down, axis=2)))
    final_down = (merged_down / jnp.expand_dims(scale_down, 2)).astype(jnp.bfloat16)
    serve_router = (router_weight * router_gain[:, None]).astype(jnp.bfloat16)
    return (final_down, scale_down, serve_router)
```

```python
import functools

import jax
import jax.numpy as jnp
from jax import lax
from jax.experimental import pallas as pl
from jax.experimental.pallas import tpu as pltpu
from jax.sharding import PartitionSpec as P

MESH = pl.DeviceIdType.MESH
SIDE = 4
LANES = 128

ROUNDS = (
    ((2, 3), (0, 1)),
    ((1, 3), (3, 1)),
    ((2, 1), (0, 3)),
    ((0, 2), (2, 0)),
    ((1, 0), (3, 2)),
    ((1, 2), (3, 0)),
    ((3, 3), (1, 1)),
    ((2, 2),),
)
DEPTH = 2


def pick(table, i):
    value = jnp.int32(0)
    for n, entry in enumerate(table):
        value = jnp.where(i == n, jnp.int32(entry), value)
    return value


def toward(shard, k):
    y, x = shard // SIDE, shard % SIDE
    return ((y + k // SIDE) % SIDE) * SIDE + (x + k % SIDE) % SIDE


def away(shard, k):
    y, x = shard // SIDE, shard % SIDE
    return ((y + SIDE - k // SIDE) % SIDE) * SIDE + (x + SIDE - k % SIDE) % SIDE


def kernel(
    shards, experts,
    master, second, weight_in, gain_in,
    final, scale, router,
    wide, narrow, ready, part, got, inverse, one_router, row_router, all_router, weight, gain,
    wide_sem, narrow_sem, weight_sem, gain_sem, part_send, part_recv, inv_send, inv_recv, row_send, row_recv, rt1_send, rt1_recv, rt2_send, rt2_recv,
):
    me = lax.axis_index("shard")
    mine = lax.axis_index("expert")
    held, rows, width = wide.shape[1:]
    groups = rows // 8

    def read(k):
        where = pl.ds(pl.multiple_of(toward(me, k) * rows, 16), rows)
        return (
            pltpu.make_async_copy(master.at[:, where, :], wide.at[k], wide_sem.at[k]),
            pltpu.make_async_copy(second.at[:, where, :], narrow.at[k], narrow_sem.at[k]),
        )

    @pl.loop(0, shards)
    def _(k):
        for copy in read(k):
            copy.start()

    read_weight = pltpu.make_async_copy(weight_in, weight, weight_sem)
    read_gain = pltpu.make_async_copy(gain_in, gain, gain_sem)
    read_weight.start()
    read_gain.start()

    barrier = pltpu.get_barrier_semaphore()

    @pl.loop(1, shards)
    def _(k):
        pl.semaphore_signal(barrier, inc=1, device_id={"shard": toward(me, k)}, device_id_type=MESH)

    @pl.loop(1, experts)
    def _(k):
        pl.semaphore_signal(barrier, inc=1, device_id={"expert": (mine + k) % experts}, device_id_type=MESH)

    read_weight.wait()
    read_gain.wait()
    mine_router = (weight[...] * gain[...]).astype(jnp.bfloat16)
    one_router[...] = mine_router
    columns = pl.ds(pl.multiple_of(me * width, LANES), width)
    row_router[:, columns] = mine_router
    pl.semaphore_wait(barrier, shards + experts - 2)

    def send_part(k):
        return pltpu.make_async_remote_copy(
            src_ref=part.at[k], dst_ref=got.at[k], send_sem=part_send.at[k], recv_sem=part_recv.at[k],
            device_id={"shard": toward(me, k)}, device_id_type=MESH,
        )

    def send_inverse(k):
        return pltpu.make_async_remote_copy(
            src_ref=inverse.at[0], dst_ref=inverse.at[k], send_sem=inv_send.at[k], recv_sem=inv_recv.at[k],
            device_id={"shard": away(me, k)}, device_id_type=MESH,
        )

    def send_rows(k):
        return pltpu.make_async_remote_copy(
            src_ref=ready.at[k], dst_ref=final.at[:, :, columns], send_sem=row_send.at[k], recv_sem=row_recv.at[k],
            device_id={"shard": toward(me, k)}, device_id_type=MESH,
        )

    def send_router(k):
        return pltpu.make_async_remote_copy(
            src_ref=one_router, dst_ref=row_router.at[:, columns], send_sem=rt1_send.at[k], recv_sem=rt1_recv.at[k],
            device_id={"shard": toward(me, k)}, device_id_type=MESH,
        )

    def send_row_router(k):
        return pltpu.make_async_remote_copy(
            src_ref=row_router, dst_ref=all_router.at[mine], send_sem=rt2_send.at[k], recv_sem=rt2_recv.at[k],
            device_id={"expert": (mine + k) % experts}, device_id_type=MESH,
        )

    lane = lax.broadcasted_iota(jnp.int32, (8, LANES), 1)
    sublane = lax.broadcasted_iota(jnp.int32, (8, LANES), 0)

    def squares(k):
        for copy in read(k):
            copy.wait()
        packed = jnp.zeros((8, LANES), jnp.float32)
        for e in range(held):
            for g in range(0, groups, 2):
                tall = pl.ds(8 * g, 16)
                merged = wide[k, e, tall, :] + narrow[k, e, tall, :].astype(jnp.float32)
                sums = jnp.sum(merged * merged, axis=1, keepdims=True)
                for h in range(2):
                    packed = jnp.where(lane == e * groups + g + h, sums[8 * h : 8 * h + 8], packed)
        part[k] = packed

    @pl.loop(1, shards)
    def _(k):
        squares(k)
        send_part(k).start()

    squares(0)

    def add(k, total):
        send_part(k).wait_recv()
        return total + got[k]

    total = lax.fori_loop(1, shards, add, part[0])
    root = jnp.sqrt(total)
    inverse[0] = 1.0 / root

    @pl.loop(1, shards)
    def _(k):
        send_inverse(k).start()

    @pl.loop(1, shards)
    def _(k):
        send_router(k).start()

    def scaled(k, store):
        factors = inverse[k]
        for e in range(held):
            for g in range(0, groups, 2):
                tall = pl.ds(8 * g, 16)
                merged = wide[k, e, tall, :] + narrow[k, e, tall, :].astype(jnp.float32)
                factor = jnp.concatenate(
                    [
                        jnp.broadcast_to(factors[:, e * groups + g + h : e * groups + g + h + 1], (8, width))
                        for h in range(2)
                    ],
                    axis=0,
                )
                store(e, tall, (merged * factor).astype(jnp.bfloat16))

    def scale_rows(k):
        def store(e, tall, value):
            ready[k, e, tall, :] = value

        scaled(k, store)

    offsets = [[dy * SIDE + dx for dy, dx in pair] for pair in ROUNDS]
    paired = [pair for pair in offsets if len(pair) == 2]
    firsts, seconds = [pair[0] for pair in paired], [pair[1] for pair in paired]
    alone = [pair[0] for pair in offsets if len(pair) == 1][0]

    def prepare(k):
        send_inverse(k).wait_recv()
        scale_rows(k)

    @pl.loop(0, len(paired))
    def _(p):
        @pl.loop(0, 2)
        def _(side):
            prepare(jnp.where(side == 0, pick(firsts, p), pick(seconds, p)))

        @pl.when(p >= DEPTH)
        def _():
            send_rows(pick(firsts, p - DEPTH)).wait_send()
            send_rows(pick(seconds, p - DEPTH)).wait_send()

        send_rows(pick(firsts, p)).start()
        send_rows(pick(seconds, p)).start()

    prepare(jnp.int32(alone))
    late = len(paired) - DEPTH
    send_rows(firsts[late]).wait_send()
    send_rows(seconds[late]).wait_send()
    send_rows(alone).start()

    @pl.loop(1, shards)
    def _(k):
        send_router(k).wait_recv()

    @pl.loop(1, experts)
    def _(k):
        send_row_router(k).start()

    all_router[mine] = row_router[...]

    def keep(e, tall, value):
        final[e, tall, columns] = value

    scaled(0, keep)

    for e in range(held):
        for c in range(0, rows, LANES):
            size = min(LANES, rows - c)
            spread = jnp.zeros((8, LANES), jnp.float32)
            for g in range(c // 8, (c + size) // 8):
                at = e * groups + g
                spread = jnp.where(lane // 8 == g - c // 8, jnp.broadcast_to(root[:, at : at + 1], (8, LANES)), spread)
            line = jnp.sum(jnp.where(sublane == lane % 8, spread, 0.0), axis=0, keepdims=True)
            scale[e : e + 1, c : c + size] = line[:, :size]

    @pl.loop(1, experts)
    def _(k):
        send_row_router(k).wait()

    router[...] = all_router[...].reshape(router.shape)

    @pl.loop(1, shards)
    def _(k):
        send_part(k).wait_send()
        send_inverse(k).wait_send()
        send_router(k).wait_send()
        send_rows(k).wait_recv()

    for p in range(late + 1, len(paired)):
        send_rows(firsts[p]).wait_send()
        send_rows(seconds[p]).wait_send()
    send_rows(alone).wait_send()


def hand_out_kernel(final, scale, router, final_out, scale_out, router_out, final_sem, scale_sem, router_sem):
    copies = [
        pltpu.make_async_copy(final, final_out, final_sem),
        pltpu.make_async_copy(scale, scale_out, scale_sem),
        pltpu.make_async_copy(router, router_out, router_sem),
    ]
    for copy in copies:
        copy.start()
    for copy in copies:
        copy.wait()


def hand_out(*arrays):
    return pl.pallas_call(
        hand_out_kernel,
        name="hand_out",
        out_shape=tuple(jax.ShapeDtypeStruct(x.shape, x.dtype) for x in arrays),
        in_specs=[pl.BlockSpec(memory_space=pltpu.VMEM)] * 3,
        out_specs=(pl.BlockSpec(memory_space=pltpu.HBM),) * 3,
        scratch_shapes=[pltpu.SemaphoreType.DMA] * 3,
        compiler_params=pltpu.CompilerParams(vmem_limit_bytes=8 * 1024 * 1024),
    )(*arrays)


def solution(mesh):
    shards, experts = mesh.shape["shard"], mesh.shape["expert"]

    def local(master, second, weight, gain):
        held, length, width = master.shape
        rows = length // shards
        dma = pltpu.SemaphoreType.DMA
        final, scale, router = pl.pallas_call(
            functools.partial(kernel, shards, experts),
            name="serve",
            out_shape=(
                jax.ShapeDtypeStruct((held, rows, width * shards), jnp.bfloat16),
                jax.ShapeDtypeStruct((held, rows), jnp.float32),
                jax.ShapeDtypeStruct((experts * held, width * shards), jnp.bfloat16),
            ),
            in_specs=[pl.BlockSpec(memory_space=pltpu.HBM)] * 4,
            out_specs=(pl.BlockSpec(memory_space=pltpu.VMEM),) * 3,
            scratch_shapes=[
                pltpu.VMEM((shards, held, rows, width), jnp.float32),
                pltpu.VMEM((shards, held, rows, width), jnp.bfloat16),
                pltpu.VMEM((shards, held, rows, width), jnp.bfloat16),
                pltpu.VMEM((shards, 8, LANES), jnp.float32),
                pltpu.VMEM((shards, 8, LANES), jnp.float32),
                pltpu.VMEM((shards, 8, LANES), jnp.float32),
                pltpu.VMEM((held, width), jnp.bfloat16),
                pltpu.VMEM((held, width * shards), jnp.bfloat16),
                pltpu.VMEM((experts, held, width * shards), jnp.bfloat16),
                pltpu.VMEM((held, width), jnp.float32),
                pltpu.VMEM((1, width), jnp.float32),
            ]
            + [dma((shards,))] * 2
            + [dma] * 2
            + [dma((shards,))] * 8
            + [dma((experts,))] * 2,
            compiler_params=pltpu.CompilerParams(
                collective_id=0, has_side_effects=True, vmem_limit_bytes=44 * 1024 * 1024
            ),
        )(*[pltpu.with_memory_space_constraint(x, pltpu.HBM) for x in (master, second, weight.T, gain[None, :])])
        final, scale, router = hand_out(final, scale, router)
        return final, scale, router.T

    return jax.shard_map(
        local,
        mesh=mesh,
        in_specs=(P("expert", None, "shard"), P("expert", None, "shard"), P("shard", "expert"), P("shard")),
        out_specs=(P("expert", "shard", None), P("expert", "shard"), P()),
        check_vma=False,
    )
```

```python
import functools

import jax
import jax.numpy as jnp
from jax import lax
from jax.experimental import pallas as pl
from jax.experimental.pallas import tpu as pltpu
from jax.sharding import PartitionSpec as P

MESH = pl.DeviceIdType.MESH
SIDE = 4
LANES = 128
HALF = LANES // 2

PIECES = ((0, 1), (0, 3), (0, 2), (1, 1), (1, 3), (1, 2), (0, 0), (1, 0))
ALONG = (1, 3, 2, 0)
STRAIGHT = (1, 3, 2, 4, 12, 8)
CUT = (0, 48, 96)


def pick(table, i):
    value = jnp.int32(0)
    for n, entry in enumerate(table):
        value = jnp.where(i == n, jnp.int32(entry), value)
    return value


def toward(shard, k):
    y, x = shard // SIDE, shard % SIDE
    return ((y + k // SIDE) % SIDE) * SIDE + (x + k % SIDE) % SIDE


def away(shard, k):
    y, x = shard // SIDE, shard % SIDE
    return ((y + SIDE - k // SIDE) % SIDE) * SIDE + (x + SIDE - k % SIDE) % SIDE


def kernel(
    shards, experts,
    master, second, weight_in, gain_in,
    final, scale, router,
    wide, narrow, ready, part, got, inverse, one_router, row_router, all_router, weight, gain, raw, stage,
    wide_sem, narrow_sem, weight_sem, gain_sem, part_send, part_recv, inv_send, inv_recv, row_send, row_recv, rt1_send, rt1_recv, rt2_send, rt2_recv,
    raw_send, raw_recv, relay_send, relay_recv,
):
    me = lax.axis_index("shard")
    mine = lax.axis_index("expert")
    held, rows, width = wide.shape[1:]
    groups = rows // 8

    def read(k):
        where = pl.ds(pl.multiple_of(toward(me, k) * rows, 16), rows)
        return (
            pltpu.make_async_copy(master.at[:, where, :], wide.at[k], wide_sem.at[k]),
            pltpu.make_async_copy(second.at[:, where, :], narrow.at[k], narrow_sem.at[k]),
        )

    @pl.loop(0, shards)
    def _(k):
        for copy in read(k):
            copy.start()

    read_weight = pltpu.make_async_copy(weight_in, weight, weight_sem)
    read_gain = pltpu.make_async_copy(gain_in, gain, gain_sem)
    read_weight.start()
    read_gain.start()

    barrier = pltpu.get_barrier_semaphore()

    @pl.loop(1, shards)
    def _(k):
        pl.semaphore_signal(barrier, inc=1, device_id={"shard": toward(me, k)}, device_id_type=MESH)

    @pl.loop(1, experts)
    def _(k):
        pl.semaphore_signal(barrier, inc=1, device_id={"expert": (mine + k) % experts}, device_id_type=MESH)

    read_weight.wait()
    read_gain.wait()
    mine_router = (weight[...] * gain[...]).astype(jnp.bfloat16)
    one_router[...] = mine_router
    columns = pl.ds(pl.multiple_of(me * width, LANES), width)
    row_router[:, columns] = mine_router

    def send_part(k):
        return pltpu.make_async_remote_copy(
            src_ref=part.at[k], dst_ref=got.at[k], send_sem=part_send.at[k], recv_sem=part_recv.at[k],
            device_id={"shard": toward(me, k)}, device_id_type=MESH,
        )

    def send_inverse(k):
        return pltpu.make_async_remote_copy(
            src_ref=inverse.at[0], dst_ref=inverse.at[k], send_sem=inv_send.at[k], recv_sem=inv_recv.at[k],
            device_id={"shard": away(me, k)}, device_id_type=MESH,
        )

    def send_straight(k, e, early=False):
        skip = CUT[2] if early else 0
        part_rows = pl.ds(skip, rows - skip)
        return pltpu.make_async_remote_copy(
            src_ref=ready.at[k, e, part_rows], dst_ref=final.at[e, part_rows, columns],
            send_sem=row_send.at[2 * k + e], recv_sem=row_recv.at[2 * k + e],
            device_id={"shard": toward(me, k)}, device_id_type=MESH,
        )

    def send_relay(k, e):
        return pltpu.make_async_remote_copy(
            src_ref=ready.at[k, e], dst_ref=stage.at[k, e],
            send_sem=relay_send.at[2 * k + e], recv_sem=relay_recv.at[2 * k + e],
            device_id={"shard": toward(me, k % SIDE)}, device_id_type=MESH,
        )

    def forward(k, e):
        origin = pl.ds(pl.multiple_of(away(me, k % SIDE) * width, LANES), width)
        return pltpu.make_async_remote_copy(
            src_ref=stage.at[k, e], dst_ref=final.at[e, :, origin],
            send_sem=row_send.at[2 * k + e], recv_sem=row_recv.at[2 * k + e],
            device_id={"shard": toward(me, k - k % SIDE)}, device_id_type=MESH,
        )

    def send_raw(n, part_number):
        k = pick(STRAIGHT, n)
        first, last = CUT[part_number], CUT[part_number + 1]
        part_rows = pl.ds(first, last - first)
        at = 2 * n + part_number
        return pltpu.make_async_remote_copy(
            src_ref=wide.at[k, 0, part_rows], dst_ref=raw.at[n, part_rows],
            send_sem=raw_send.at[at], recv_sem=raw_recv.at[at],
            device_id={"shard": toward(me, k)}, device_id_type=MESH,
        )

    def send_router(k):
        return pltpu.make_async_remote_copy(
            src_ref=one_router, dst_ref=row_router.at[:, columns], send_sem=rt1_send.at[k], recv_sem=rt1_recv.at[k],
            device_id={"shard": toward(me, k)}, device_id_type=MESH,
        )

    def send_row_router(k):
        return pltpu.make_async_remote_copy(
            src_ref=row_router, dst_ref=all_router.at[mine], send_sem=rt2_send.at[k], recv_sem=rt2_recv.at[k],
            device_id={"expert": (mine + k) % experts}, device_id_type=MESH,
        )

    lane = lax.broadcasted_iota(jnp.int32, (8, LANES), 1)
    sublane = lax.broadcasted_iota(jnp.int32, (8, LANES), 0)

    def squares(k):
        for copy in read(k):
            copy.wait()
        packed = jnp.zeros((8, LANES), jnp.float32)
        for e in range(held):
            for g in range(0, groups, 2):
                tall = pl.ds(8 * g, 16)
                merged = wide[k, e, tall, :] + narrow[k, e, tall, :].astype(jnp.float32)
                sums = jnp.sum(merged * merged, axis=1, keepdims=True)
                for h in range(2):
                    packed = jnp.where(lane == e * HALF + g + h, sums[8 * h : 8 * h + 8], packed)
        part[k] = packed

    @pl.loop(1, shards // 2)
    def _(k):
        squares(k)

    pl.semaphore_wait(barrier, shards + experts - 2)

    @pl.loop(1, shards // 2)
    def _(k):
        send_part(k).start()

    @pl.loop(shards // 2, shards)
    def _(k):
        squares(k)
        send_part(k).start()

    @pl.loop(0, len(STRAIGHT))
    def _(n):
        k = pick(STRAIGHT, n)
        for g in range(0, CUT[2] // 8, 2):
            tall = pl.ds(8 * g, 16)
            wide[k, 0, tall, :] += narrow[k, 0, tall, :].astype(jnp.float32)

    squares(0)

    @pl.loop(0, len(STRAIGHT))
    def _(n):
        send_raw(n, 0).start()

    def add(k, total):
        send_part(k).wait_recv()
        return total + got[k]

    total = lax.fori_loop(1, shards, add, part[0])
    root = jnp.sqrt(total)
    inverse[0] = 1.0 / root

    @pl.loop(1, shards)
    def _(k):
        send_inverse(k).start()

    @pl.loop(0, len(STRAIGHT))
    def _(n):
        send_raw(n, 1).start()

    @pl.loop(1, shards)
    def _(k):
        send_router(k).start()

    def factor_of(factors, g):
        return jnp.concatenate([jnp.broadcast_to(factors[:, a : a + 1], (8, width)) for a in (g, g + 1)], axis=0)

    def scaled(k, e, store):
        both = inverse[k]
        factors = jnp.where(e == 0, both, pltpu.roll(both, HALF, 1))
        for g in range(0, groups, 2):
            tall = pl.ds(8 * g, 16)
            merged = wide[k, e, tall, :] + narrow[k, e, tall, :].astype(jnp.float32)
            store(tall, (merged * factor_of(factors, g)).astype(jnp.bfloat16))

    experts_of, dys_of = [e for e, dy in PIECES], [dy for e, dy in PIECES]

    @pl.loop(0, len(PIECES) * SIDE)
    def _(i):
        e, dy, dx = pick(experts_of, i // SIDE), pick(dys_of, i // SIDE), pick(ALONG, i % SIDE)
        k = dy * SIDE + dx

        @pl.when(k != 0)
        def _():
            @pl.when(e == 0)
            def _():
                send_inverse(k).wait_recv()

            def store(tall, value):
                ready[k, e, tall, :] = value

            scaled(k, e, store)

            @pl.when((dy != 0) & (dx != 0))
            def _():
                send_relay(k, e).start()

            @pl.when(((dy == 0) | (dx == 0)) & (e == 0))
            def _():
                send_straight(k, 0, True).start()

            @pl.when(((dy == 0) | (dx == 0)) & (e != 0))
            def _():
                send_straight(k, 1).start()

    @pl.loop(1, shards)
    def _(k):
        send_router(k).wait_recv()

    @pl.loop(1, experts)
    def _(k):
        send_row_router(k).start()

    @pl.loop(0, (len(PIECES) - held) * (SIDE - 1))
    def _(i):
        e, dy, dx = pick(experts_of, i // 3), pick(dys_of, i // 3), pick(ALONG, i % 3)
        k = dy * SIDE + dx
        send_relay(k, e).wait_recv()
        forward(k, e).start()

    all_router[mine] = row_router[...]

    @pl.loop(0, held)
    def _(e):
        def keep(tall, value):
            final[e, tall, columns] = value

        scaled(0, e, keep)

    factors = inverse[0]

    @pl.loop(0, len(STRAIGHT))
    def _(n):
        send_raw(n, 0).wait_recv()
        send_raw(n, 1).wait_recv()
        origin = pl.ds(pl.multiple_of(away(me, pick(STRAIGHT, n)) * width, LANES), width)
        for g in range(0, CUT[2] // 8, 2):
            tall = pl.ds(8 * g, 16)
            final[0, tall, origin] = (raw[n, tall, :] * factor_of(factors, g)).astype(jnp.bfloat16)

    for e in range(held):
        for c in range(0, rows, LANES):
            size = min(LANES, rows - c)
            spread = jnp.zeros((8, LANES), jnp.float32)
            for g in range(c // 8, (c + size) // 8):
                at = e * HALF + g
                spread = jnp.where(lane // 8 == g - c // 8, jnp.broadcast_to(root[:, at : at + 1], (8, LANES)), spread)
            line = jnp.sum(jnp.where(sublane == lane % 8, spread, 0.0), axis=0, keepdims=True)
            scale[e : e + 1, c : c + size] = line[:, :size]

    @pl.loop(1, experts)
    def _(k):
        send_row_router(k).wait()

    router[...] = all_router[...].reshape(router.shape)

    @pl.loop(1, shards)
    def _(k):
        send_part(k).wait_send()
        send_inverse(k).wait_send()
        send_router(k).wait_send()

    @pl.loop(0, len(STRAIGHT))
    def _(n):
        k = pick(STRAIGHT, n)
        send_raw(n, 0).wait_send()
        send_raw(n, 1).wait_send()
        send_straight(k, 0, True).wait()
        send_straight(k, 1).wait()

    @pl.loop(0, (len(PIECES) - held) * (SIDE - 1))
    def _(i):
        e, dy, dx = pick(experts_of, i // 3), pick(dys_of, i // 3), pick(ALONG, i % 3)
        k = dy * SIDE + dx
        send_relay(k, e).wait_send()
        forward(k, e).wait()


def hand_out_kernel(final, scale, router, final_out, scale_out, router_out, final_sem, scale_sem, router_sem):
    copies = [
        pltpu.make_async_copy(final, final_out, final_sem),
        pltpu.make_async_copy(scale, scale_out, scale_sem),
        pltpu.make_async_copy(router, router_out, router_sem),
    ]
    for copy in copies:
        copy.start()
    for copy in copies:
        copy.wait()


def hand_out(*arrays):
    return pl.pallas_call(
        hand_out_kernel,
        name="hand_out",
        out_shape=tuple(jax.ShapeDtypeStruct(x.shape, x.dtype) for x in arrays),
        in_specs=[pl.BlockSpec(memory_space=pltpu.VMEM)] * 3,
        out_specs=(pl.BlockSpec(memory_space=pltpu.HBM),) * 3,
        scratch_shapes=[pltpu.SemaphoreType.DMA] * 3,
        compiler_params=pltpu.CompilerParams(vmem_limit_bytes=8 * 1024 * 1024),
    )(*arrays)


def solution(mesh):
    shards, experts = mesh.shape["shard"], mesh.shape["expert"]

    def local(master, second, weight, gain):
        held, length, width = master.shape
        rows = length // shards
        dma = pltpu.SemaphoreType.DMA
        final, scale, router = pl.pallas_call(
            functools.partial(kernel, shards, experts),
            name="serve",
            out_shape=(
                jax.ShapeDtypeStruct((held, rows, width * shards), jnp.bfloat16),
                jax.ShapeDtypeStruct((held, rows), jnp.float32),
                jax.ShapeDtypeStruct((experts * held, width * shards), jnp.bfloat16),
            ),
            in_specs=[pl.BlockSpec(memory_space=pltpu.HBM)] * 4,
            out_specs=(pl.BlockSpec(memory_space=pltpu.VMEM),) * 3,
            scratch_shapes=[
                pltpu.VMEM((shards, held, rows, width), jnp.float32),
                pltpu.VMEM((shards, held, rows, width), jnp.bfloat16),
                pltpu.VMEM((shards, held, rows, width), jnp.bfloat16),
                pltpu.VMEM((shards, 8, LANES), jnp.float32),
                pltpu.VMEM((shards, 8, LANES), jnp.float32),
                pltpu.VMEM((shards, 8, LANES), jnp.float32),
                pltpu.VMEM((held, width), jnp.bfloat16),
                pltpu.VMEM((held, width * shards), jnp.bfloat16),
                pltpu.VMEM((experts, held, width * shards), jnp.bfloat16),
                pltpu.VMEM((held, width), jnp.float32),
                pltpu.VMEM((1, width), jnp.float32),
                pltpu.VMEM((len(STRAIGHT), CUT[2], width), jnp.float32),
                pltpu.VMEM((shards, held, rows, width), jnp.bfloat16),
            ]
            + [dma((shards,))] * 2
            + [dma] * 2
            + [dma((shards,))] * 4
            + [dma((held * shards,))] * 2
            + [dma((shards,))] * 2
            + [dma((experts,))] * 2
            + [dma((2 * len(STRAIGHT),))] * 2
            + [dma((held * shards,))] * 2,
            compiler_params=pltpu.CompilerParams(
                collective_id=0, has_side_effects=True, vmem_limit_bytes=44 * 1024 * 1024
            ),
        )(*[pltpu.with_memory_space_constraint(x, pltpu.HBM) for x in (master, second, weight.T, gain[None, :])])
        final, scale, router = hand_out(final, scale, router)
        return final, scale, router.T

    return jax.shard_map(
        local,
        mesh=mesh,
        in_specs=(P("expert", None, "shard"), P("expert", None, "shard"), P("shard", "expert"), P("shard")),
        out_specs=(P("expert", "shard", None), P("expert", "shard"), P()),
        check_vma=False,
    )
```

```python
import functools

import jax
import jax.numpy as jnp
from jax import lax
from jax.experimental import pallas as pl
from jax.experimental.pallas import tpu as pltpu
from jax.sharding import PartitionSpec as P

MESH = pl.DeviceIdType.MESH
SIDE = 4
LANES = 128
HALF = LANES // 2
PIECE = 80

RELAYED = ((5, 15, 10), (7, 14, 9), (11, 6, 13))
ALONG_X = (2, 1, 3)
ALONG_Y = (4, 12, 8)
GROUP = tuple(next((n for n, group in enumerate(RELAYED) if k in group), 0) for k in range(SIDE * SIDE))
FIRST = 128
SLOT = FIRST // 8


def pick(table, i):
    value = jnp.int32(table[0])
    for n, entry in enumerate(table[1:], 1):
        value = jnp.where(i == n, jnp.int32(entry), value)
    return value


def toward(shard, k):
    y, x = lax.div(shard, SIDE), lax.rem(shard, SIDE)
    return lax.rem(y + lax.div(k, SIDE), SIDE) * SIDE + lax.rem(x + lax.rem(k, SIDE), SIDE)


def away(shard, k):
    y, x = lax.div(shard, SIDE), lax.rem(shard, SIDE)
    return lax.rem(y + SIDE - lax.div(k, SIDE), SIDE) * SIDE + lax.rem(x + SIDE - lax.rem(k, SIDE), SIDE)


def kernel(
    shards, experts,
    master, second, weight_in, gain_in,
    final, scale, router,
    wide, narrow, ready, stage, first_got, first_total, first_inverse, part, got, rest_total, inverse,
    one_router, row_router, all_router, weight, gain,
    first_read, rest_read, weight_read, gain_read, first_send, first_recv, part_send, part_recv, inv_send, inv_recv,
    rt1_send, rt1_recv, rt2_send, rt2_recv, relay_recv, row_send, forward_send, row_recv,
):
    me = lax.axis_index("shard")
    mine = lax.axis_index("expert")
    held, rows, width = wide.shape[1:]
    columns = pl.ds(pl.multiple_of(me * width, LANES), width)
    chunks = ((0, 0, FIRST), (0, FIRST, rows - FIRST)) + tuple((e, 0, rows) for e in range(1, held))

    def local(ref, sem):
        return pltpu.make_async_copy(ref, ref, sem)

    def read(k, c, sem):
        e, start, count = chunks[c]
        source = pl.ds(pl.multiple_of(toward(me, k) * rows + start, 16), count)
        target = pl.ds(start, count)
        pltpu.make_async_copy(master.at[e, source], wide.at[k, e, target], sem).start()
        pltpu.make_async_copy(second.at[e, source], narrow.at[k, e, target], sem).start()

    read_weight = pltpu.make_async_copy(weight_in, weight, weight_read)
    read_gain = pltpu.make_async_copy(gain_in, gain, gain_read)
    read_weight.start()
    read_gain.start()

    barrier = pltpu.get_barrier_semaphore()

    @pl.loop(1, shards)
    def _(k):
        pl.semaphore_signal(barrier, inc=1, device_id={"shard": toward(me, k)}, device_id_type=MESH)

    @pl.loop(1, experts)
    def _(k):
        pl.semaphore_signal(barrier, inc=1, device_id={"expert": lax.rem(mine + k, experts)}, device_id_type=MESH)

    @pl.loop(0, shards)
    def _(k):
        read(k, 0, first_read)

    @pl.loop(1, shards + 1)
    def _(k):
        for c in range(1, len(chunks)):
            read(lax.rem(k, shards), c, rest_read.at[lax.rem(k, shards)])

    lane = lax.broadcasted_iota(jnp.int32, (8, LANES), 1)
    sublane = lax.broadcasted_iota(jnp.int32, (8, LANES), 0)

    def sums_of(k, c, packed, base):
        e, start, count = chunks[c]
        for g in range(start // 8, (start + count) // 8, 2):
            tall = pl.ds(8 * g, 16)
            merged = wide[k, e, tall, :] + narrow[k, e, tall, :].astype(jnp.float32)
            sums = jnp.sum(merged * merged, axis=1, keepdims=True)
            for h in range(2):
                packed = jnp.where(lane == base + g + h, sums[8 * h : 8 * h + 8], packed)
        return packed

    local(narrow.at[:, 0, pl.ds(0, 3 * FIRST)], first_read).wait()

    def first_sums(i, packed):
        for k in [4 * i + n for n in range(4)]:
            owner = toward(me, k)
            base = lax.rem(owner, 8) * SLOT
            low = owner < 8
            sums = sums_of(k, 0, zero, base)
            packed = packed[0] + jnp.where(low, sums, 0.0), packed[1] + jnp.where(low, 0.0, sums)
        return packed

    zero = jnp.zeros((8, LANES), jnp.float32)
    packed = lax.fori_loop(0, shards // 4, first_sums, (zero, zero))
    first_got[me, 0] = packed[0]
    first_got[me, 1] = packed[1]
    pl.semaphore_wait(barrier, shards + experts - 2)

    @pl.loop(1, shards)
    def _(k):
        pltpu.make_async_remote_copy(
            src_ref=first_got.at[me], dst_ref=first_got.at[me], send_sem=first_send, recv_sem=first_recv,
            device_id={"shard": toward(me, k)}, device_id_type=MESH,
        ).start()

    read_weight.wait()
    read_gain.wait()
    mine_router = (weight[...] * gain[...]).astype(jnp.bfloat16)
    one_router[...] = mine_router
    row_router[:, columns] = mine_router

    @pl.loop(1, shards)
    def _(k):
        pltpu.make_async_remote_copy(
            src_ref=one_router, dst_ref=row_router.at[:, columns], send_sem=rt1_send, recv_sem=rt1_recv,
            device_id={"shard": toward(me, k)}, device_id_type=MESH,
        ).start()

    def rest_sums(k):
        local(narrow.at[pl.ds(0, 3), :, pl.ds(0, (held * rows - FIRST) // held)], rest_read.at[k]).wait()
        packed = zero
        for c in range(1, len(chunks)):
            packed = sums_of(k, c, packed, chunks[c][0] * HALF)
        part[k] = packed

    @pl.loop(1, shards)
    def _(k):
        rest_sums(k)
        pltpu.make_async_remote_copy(
            src_ref=part.at[k], dst_ref=got.at[k], send_sem=part_send, recv_sem=part_recv,
            device_id={"shard": toward(me, k)}, device_id_type=MESH,
        ).start()

    rest_sums(0)

    local(first_got.at[pl.ds(0, shards - 1)], first_recv).wait()
    for v in range(2):
        total = first_got[0, v]
        for d in range(1, shards):
            total += first_got[d, v]
        first_total[v] = total
        first_inverse[v] = 1.0 / jnp.sqrt(total)

    def of_owner(ref, owner):
        return pltpu.roll(ref[lax.div(owner, 8)], LANES - lax.rem(owner, 8) * SLOT, 1)

    def scaled(k, c, store):
        e, start, count = chunks[c]
        factors = of_owner(first_inverse, toward(me, k)) if c == 0 else inverse[k]
        for g in range(start // 8, (start + count) // 8, 2):
            tall = pl.ds(8 * g, 16)
            merged = wide[k, e, tall, :] + narrow[k, e, tall, :].astype(jnp.float32)
            at = [e * HALF + g + h for h in range(2)]
            factor = jnp.concatenate([jnp.broadcast_to(factors[:, a : a + 1], (8, width)) for a in at], axis=0)
            store(e, tall, (merged * factor).astype(jnp.bfloat16))

    def send_pieces(c, offsets):
        e, start, count = chunks[c]
        part_rows = pl.ds(start, count)

        @pl.loop(0, len(offsets))
        def _(i):
            k = pick(offsets, i)
            dy, dx = lax.div(k, SIDE), lax.rem(k, SIDE)

            if c == held:
                local(inverse.at[k], inv_recv.at[k]).wait()

            def store(e, tall, value):
                ready[k, e, tall, :] = value

            scaled(k, c, store)

            @pl.when((dy != 0) & (dx != 0))
            def _():
                pltpu.make_async_remote_copy(
                    src_ref=ready.at[k, e, part_rows], dst_ref=stage.at[k, e, part_rows],
                    send_sem=row_send, recv_sem=relay_recv.at[c * SIDE + pick(GROUP, k)],
                    device_id={"shard": toward(me, dx)}, device_id_type=MESH,
                ).start()

            @pl.when((dy == 0) | (dx == 0))
            def _():
                pltpu.make_async_remote_copy(
                    src_ref=ready.at[k, e, part_rows], dst_ref=final.at[e, part_rows, columns],
                    send_sem=row_send, recv_sem=row_recv,
                    device_id={"shard": toward(me, k)}, device_id_type=MESH,
                ).start()

    def forward_groups(c, begin, end):
        e, start, count = chunks[c]
        part_rows = pl.ds(start, count)

        @pl.loop(begin, end)
        def _(i):
            local(stage.at[pl.ds(0, SIDE - 1), e, part_rows], relay_recv.at[c * SIDE + i]).wait()

            @pl.loop(0, SIDE - 1)
            def _(j):
                k = pick(sum(RELAYED, ()), i * (SIDE - 1) + j)
                origin = pl.ds(pl.multiple_of(away(me, lax.rem(k, SIDE)) * width, LANES), width)
                pltpu.make_async_remote_copy(
                    src_ref=stage.at[k, e, part_rows], dst_ref=final.at[e, part_rows, origin],
                    send_sem=forward_send, recv_sem=row_recv,
                    device_id={"shard": toward(me, k - lax.rem(k, SIDE))}, device_id_type=MESH,
                ).start()

    send_pieces(0, RELAYED[0] + ALONG_Y)

    local(got.at[pl.ds(1, shards - 1)], part_recv).wait()
    total = part[0]
    for k in range(1, shards):
        total += got[k]
    rest_total[...] = total
    inverse[0] = 1.0 / jnp.sqrt(total)

    @pl.loop(1, shards)
    def _(k):
        pltpu.make_async_remote_copy(
            src_ref=inverse.at[0], dst_ref=inverse.at[k], send_sem=inv_send, recv_sem=inv_recv.at[k],
            device_id={"shard": away(me, k)}, device_id_type=MESH,
        ).start()

    send_pieces(0, RELAYED[1] + RELAYED[2] + ALONG_X)
    others = row_router.at[:, pl.ds(0, (shards - 1) * width)]
    local(others, rt1_recv).wait()

    @pl.loop(1, experts)
    def _(k):
        pltpu.make_async_remote_copy(
            src_ref=row_router, dst_ref=all_router.at[mine], send_sem=rt2_send, recv_sem=rt2_recv,
            device_id={"expert": lax.rem(mine + k, experts)}, device_id_type=MESH,
        ).start()

    all_router[mine] = row_router[...]

    forward_groups(0, 0, 3)
    late = range(len(chunks) - 1, 0, -1)
    for c in late:
        send_pieces(c, RELAYED[0] + ALONG_Y + RELAYED[1] + RELAYED[2])

    for c in late[:-1]:
        forward_groups(c, 0, 3)
    forward_groups(late[-1], 0, 2)
    for c in late:
        send_pieces(c, ALONG_X)
    forward_groups(late[-1], 2, 3)

    def keep(e, tall, value):
        final[e, tall, columns] = value

    for c in range(len(chunks)):
        scaled(0, c, keep)

    root = jnp.sqrt(jnp.where(lane < SLOT, of_owner(first_total, me), rest_total[...]))
    for e in range(held):
        for c in range(0, rows, LANES):
            size = min(LANES, rows - c)
            spread = jnp.zeros((8, LANES), jnp.float32)
            for g in range(c // 8, (c + size) // 8):
                at = e * HALF + g
                spread = jnp.where(lane // 8 == g - c // 8, jnp.broadcast_to(root[:, at : at + 1], (8, LANES)), spread)
            line = jnp.sum(jnp.where(sublane == lane % 8, spread, 0.0), axis=0, keepdims=True)
            scale[e : e + 1, c : c + size] = line[:, :size]

    local(all_router.at[pl.ds(0, experts - 1)], rt2_recv).wait()
    router[...] = all_router[...].reshape(router.shape)

    local(first_got.at[pl.ds(0, shards - 1)], first_send).wait()
    local(part.at[pl.ds(1, shards - 1)], part_send).wait()
    local(got.at[pl.ds(1, shards - 1)], inv_send).wait()
    local(others, rt1_send).wait()
    local(all_router.at[pl.ds(0, experts - 1)], rt2_send).wait()
    local(ready.at[pl.ds(1, shards - 1)], row_send).wait()
    local(ready.at[pl.ds(0, (SIDE - 1) * (SIDE - 1))], forward_send).wait()
    local(ready.at[pl.ds(1, shards - 1)], row_recv).wait()


def hand_out_kernel(final, scale, router, final_out, scale_out, router_out, sem):
    copies = [(scale, scale_out), (router, router_out)]
    held, rows, _ = final.shape
    for e in range(held):
        for start in range(0, rows, PIECE):
            at = (e, pl.ds(start, min(PIECE, rows - start)))
            copies.append((final.at[at], final_out.at[at]))
    copies = [pltpu.make_async_copy(source, target, sem.at[n]) for n, (source, target) in enumerate(copies)]
    for copy in copies:
        copy.start()
    for copy in copies:
        copy.wait()


def hand_out(*arrays):
    held, rows, _ = arrays[0].shape
    return pl.pallas_call(
        hand_out_kernel,
        name="hand_out",
        out_shape=tuple(jax.ShapeDtypeStruct(x.shape, x.dtype) for x in arrays),
        in_specs=[pl.BlockSpec(memory_space=pltpu.VMEM)] * 3,
        out_specs=(pl.BlockSpec(memory_space=pltpu.HBM),) * 3,
        scratch_shapes=[pltpu.SemaphoreType.DMA((2 + held * pl.cdiv(rows, PIECE),))],
        compiler_params=pltpu.CompilerParams(vmem_limit_bytes=8 * 1024 * 1024),
    )(*arrays)


def solution(mesh):
    shards, experts = mesh.shape["shard"], mesh.shape["expert"]

    def local(master, second, weight, gain):
        held, length, width = master.shape
        rows = length // shards
        dma = pltpu.SemaphoreType.DMA
        wide = (shards, held, rows, width)
        final, scale, router = pl.pallas_call(
            functools.partial(kernel, shards, experts),
            name="serve",
            out_shape=(
                jax.ShapeDtypeStruct((held, rows, width * shards), jnp.bfloat16),
                jax.ShapeDtypeStruct((held, rows), jnp.float32),
                jax.ShapeDtypeStruct((experts * held, width * shards), jnp.bfloat16),
            ),
            in_specs=[pl.BlockSpec(memory_space=pltpu.HBM)] * 4,
            out_specs=(pl.BlockSpec(memory_space=pltpu.VMEM),) * 3,
            scratch_shapes=[
                pltpu.VMEM(wide, jnp.float32),
                pltpu.VMEM(wide, jnp.bfloat16),
                pltpu.VMEM(wide, jnp.bfloat16),
                pltpu.VMEM(wide, jnp.bfloat16),
                pltpu.VMEM((shards, 2, 8, LANES), jnp.float32),
                pltpu.VMEM((2, 8, LANES), jnp.float32),
                pltpu.VMEM((2, 8, LANES), jnp.float32),
                pltpu.VMEM((shards, 8, LANES), jnp.float32),
                pltpu.VMEM((shards, 8, LANES), jnp.float32),
                pltpu.VMEM((8, LANES), jnp.float32),
                pltpu.VMEM((shards, 8, LANES), jnp.float32),
                pltpu.VMEM((held, width), jnp.bfloat16),
                pltpu.VMEM((held, width * shards), jnp.bfloat16),
                pltpu.VMEM((experts, held, width * shards), jnp.bfloat16),
                pltpu.VMEM((held, width), jnp.float32),
                pltpu.VMEM((1, width), jnp.float32),
                dma, dma((shards,)), dma, dma, dma, dma, dma, dma, dma, dma((shards,)),
                dma, dma, dma, dma, dma(((held + 1) * SIDE,)), dma, dma, dma,
            ],
            compiler_params=pltpu.CompilerParams(
                collective_id=0, has_side_effects=True, vmem_limit_bytes=44 * 1024 * 1024
            ),
        )(*[pltpu.with_memory_space_constraint(x, pltpu.HBM) for x in (master, second, weight.T, gain[None, :])])
        final, scale, router = hand_out(final, scale, router)
        return final, scale, router.T

    return jax.shard_map(
        local,
        mesh=mesh,
        in_specs=(P("expert", None, "shard"), P("expert", None, "shard"), P("shard", "expert"), P("shard")),
        out_specs=(P("expert", "shard", None), P("expert", "shard"), P()),
        check_vma=False,
    )
```

```python
import functools

import jax
import jax.numpy as jnp
from jax import lax
from jax.experimental import pallas as pl
from jax.experimental.pallas import tpu as pltpu
from jax.sharding import PartitionSpec as P

MESH = pl.DeviceIdType.MESH
SIDE = 4
LANES = 128
HALF = LANES // 2
PIECE = 80

RELAYED = ((5, 15, 10), (7, 14, 9), (11, 6, 13))
Y_FIRST = ((1,), (1,), (1,))
ALONG_X = (2, 1, 3)
ALONG_Y = (4, 12, 8)
GROUP = tuple(next((n for n, group in enumerate(RELAYED) if k in group), 0) for k in range(SIDE * SIDE))
FIRST = 128
SLOT = FIRST // 8


def pick(table, i):
    value = jnp.int32(table[0])
    for n, entry in enumerate(table[1:], 1):
        value = jnp.where(i == n, jnp.int32(entry), value)
    return value


def toward(shard, k):
    y, x = lax.div(shard, SIDE), lax.rem(shard, SIDE)
    return lax.rem(y + lax.div(k, SIDE), SIDE) * SIDE + lax.rem(x + lax.rem(k, SIDE), SIDE)


def away(shard, k):
    y, x = lax.div(shard, SIDE), lax.rem(shard, SIDE)
    return lax.rem(y + SIDE - lax.div(k, SIDE), SIDE) * SIDE + lax.rem(x + SIDE - lax.rem(k, SIDE), SIDE)


def kernel(
    shards, experts,
    master, second, weight_in, gain_in,
    final, scale, router,
    wide, narrow, ready, stage, first_got, first_total, first_inverse, part, got, rest_total, inverse,
    one_router, row_router, all_router, weight, gain,
    first_read, rest_read, weight_read, gain_read, first_send, first_recv, part_send, part_recv, inv_send, inv_recv,
    rt1_send, rt1_recv, rt2_send, rt2_recv, relay_recv, row_send, forward_send, row_recv,
):
    me = lax.axis_index("shard")
    mine = lax.axis_index("expert")
    held, rows, width = wide.shape[1:]
    columns = pl.ds(pl.multiple_of(me * width, LANES), width)
    chunks = ((0, 0, FIRST), (0, FIRST, rows - FIRST)) + tuple((e, 0, rows) for e in range(1, held))

    def local(ref, sem):
        return pltpu.make_async_copy(ref, ref, sem)

    def read(k, c, sem):
        e, start, count = chunks[c]
        source = pl.ds(pl.multiple_of(toward(me, k) * rows + start, 16), count)
        target = pl.ds(start, count)
        pltpu.make_async_copy(master.at[e, source], wide.at[k, e, target], sem).start()
        pltpu.make_async_copy(second.at[e, source], narrow.at[k, e, target], sem).start()

    read_weight = pltpu.make_async_copy(weight_in, weight, weight_read)
    read_gain = pltpu.make_async_copy(gain_in, gain, gain_read)
    read_weight.start()
    read_gain.start()

    barrier = pltpu.get_barrier_semaphore()

    @pl.loop(1, shards)
    def _(k):
        pl.semaphore_signal(barrier, inc=1, device_id={"shard": toward(me, k)}, device_id_type=MESH)

    @pl.loop(1, experts)
    def _(k):
        pl.semaphore_signal(barrier, inc=1, device_id={"expert": lax.rem(mine + k, experts)}, device_id_type=MESH)

    @pl.loop(0, shards)
    def _(k):
        read(k, 0, first_read)

    @pl.loop(1, shards + 1)
    def _(k):
        for c in range(1, len(chunks)):
            read(lax.rem(k, shards), c, rest_read.at[lax.rem(k, shards)])

    lane = lax.broadcasted_iota(jnp.int32, (8, LANES), 1)
    sublane = lax.broadcasted_iota(jnp.int32, (8, LANES), 0)

    def sums_of(k, c, packed, base):
        e, start, count = chunks[c]
        for g in range(start // 8, (start + count) // 8, 2):
            tall = pl.ds(8 * g, 16)
            merged = wide[k, e, tall, :] + narrow[k, e, tall, :].astype(jnp.float32)
            sums = jnp.sum(merged * merged, axis=1, keepdims=True)
            for h in range(2):
                packed = jnp.where(lane == base + g + h, sums[8 * h : 8 * h + 8], packed)
        return packed

    local(narrow.at[:, 0, pl.ds(0, 3 * FIRST)], first_read).wait()

    def first_sums(i, packed):
        for k in [4 * i + n for n in range(4)]:
            owner = toward(me, k)
            base = lax.rem(owner, 8) * SLOT
            low = owner < 8
            sums = sums_of(k, 0, zero, base)
            packed = packed[0] + jnp.where(low, sums, 0.0), packed[1] + jnp.where(low, 0.0, sums)
        return packed

    zero = jnp.zeros((8, LANES), jnp.float32)
    packed = lax.fori_loop(0, shards // 4, first_sums, (zero, zero))
    first_got[me, 0] = packed[0]
    first_got[me, 1] = packed[1]
    pl.semaphore_wait(barrier, shards + experts - 2)

    @pl.loop(1, shards)
    def _(k):
        pltpu.make_async_remote_copy(
            src_ref=first_got.at[me], dst_ref=first_got.at[me], send_sem=first_send, recv_sem=first_recv,
            device_id={"shard": toward(me, k)}, device_id_type=MESH,
        ).start()

    read_weight.wait()
    read_gain.wait()
    mine_router = (weight[...] * gain[...]).astype(jnp.bfloat16)
    one_router[...] = mine_router
    row_router[:, columns] = mine_router

    @pl.loop(1, shards)
    def _(k):
        pltpu.make_async_remote_copy(
            src_ref=one_router, dst_ref=row_router.at[:, columns], send_sem=rt1_send, recv_sem=rt1_recv,
            device_id={"shard": toward(me, k)}, device_id_type=MESH,
        ).start()

    def rest_sums(k):
        local(narrow.at[pl.ds(0, 3), :, pl.ds(0, (held * rows - FIRST) // held)], rest_read.at[k]).wait()
        packed = zero
        for c in range(1, len(chunks)):
            packed = sums_of(k, c, packed, chunks[c][0] * HALF)
        part[k] = packed

    @pl.loop(1, shards)
    def _(k):
        rest_sums(k)
        pltpu.make_async_remote_copy(
            src_ref=part.at[k], dst_ref=got.at[k], send_sem=part_send, recv_sem=part_recv,
            device_id={"shard": toward(me, k)}, device_id_type=MESH,
        ).start()

    rest_sums(0)

    local(first_got.at[pl.ds(0, shards - 1)], first_recv).wait()
    for v in range(2):
        total = first_got[0, v]
        for d in range(1, shards):
            total += first_got[d, v]
        first_total[v] = total
        first_inverse[v] = 1.0 / jnp.sqrt(total)

    def of_owner(ref, owner):
        return pltpu.roll(ref[lax.div(owner, 8)], LANES - lax.rem(owner, 8) * SLOT, 1)

    def scaled(k, c, store):
        e, start, count = chunks[c]
        factors = of_owner(first_inverse, toward(me, k)) if c == 0 else inverse[k]
        for g in range(start // 8, (start + count) // 8, 2):
            tall = pl.ds(8 * g, 16)
            merged = wide[k, e, tall, :] + narrow[k, e, tall, :].astype(jnp.float32)
            at = [e * HALF + g + h for h in range(2)]
            factor = jnp.concatenate([jnp.broadcast_to(factors[:, a : a + 1], (8, width)) for a in at], axis=0)
            store(e, tall, (merged * factor).astype(jnp.bfloat16))

    def first_hop(c, k):
        swapped = sum([RELAYED[n] for n in Y_FIRST[c]], ())
        return pick([n - n % SIDE if n in swapped else n % SIDE for n in range(shards)], k)

    def send_pieces(c, offsets):
        e, start, count = chunks[c]
        part_rows = pl.ds(start, count)

        @pl.loop(0, len(offsets))
        def _(i):
            k = pick(offsets, i)
            dy, dx = lax.div(k, SIDE), lax.rem(k, SIDE)

            if c == held:
                local(inverse.at[k], inv_recv.at[k]).wait()

            def store(e, tall, value):
                ready[k, e, tall, :] = value

            scaled(k, c, store)

            @pl.when((dy != 0) & (dx != 0))
            def _():
                pltpu.make_async_remote_copy(
                    src_ref=ready.at[k, e, part_rows], dst_ref=stage.at[k, e, part_rows],
                    send_sem=row_send, recv_sem=relay_recv.at[c * SIDE + pick(GROUP, k)],
                    device_id={"shard": toward(me, first_hop(c, k))}, device_id_type=MESH,
                ).start()

            @pl.when((dy == 0) | (dx == 0))
            def _():
                pltpu.make_async_remote_copy(
                    src_ref=ready.at[k, e, part_rows], dst_ref=final.at[e, part_rows, columns],
                    send_sem=row_send, recv_sem=row_recv,
                    device_id={"shard": toward(me, k)}, device_id_type=MESH,
                ).start()

    def forward_groups(c, begin, end):
        e, start, count = chunks[c]
        part_rows = pl.ds(start, count)

        @pl.loop(begin, end)
        def _(i):
            local(stage.at[pl.ds(0, SIDE - 1), e, part_rows], relay_recv.at[c * SIDE + i]).wait()

            @pl.loop(0, SIDE - 1)
            def _(j):
                k = pick(sum(RELAYED, ()), i * (SIDE - 1) + j)
                hop = first_hop(c, k)
                origin = pl.ds(pl.multiple_of(away(me, hop) * width, LANES), width)
                pltpu.make_async_remote_copy(
                    src_ref=stage.at[k, e, part_rows], dst_ref=final.at[e, part_rows, origin],
                    send_sem=forward_send, recv_sem=row_recv,
                    device_id={"shard": toward(me, k - hop)}, device_id_type=MESH,
                ).start()

    send_pieces(0, RELAYED[0] + ALONG_Y)

    local(got.at[pl.ds(1, shards - 1)], part_recv).wait()
    total = part[0]
    for k in range(1, shards):
        total += got[k]
    rest_total[...] = total
    inverse[0] = 1.0 / jnp.sqrt(total)

    @pl.loop(1, shards)
    def _(k):
        pltpu.make_async_remote_copy(
            src_ref=inverse.at[0], dst_ref=inverse.at[k], send_sem=inv_send, recv_sem=inv_recv.at[k],
            device_id={"shard": away(me, k)}, device_id_type=MESH,
        ).start()

    send_pieces(0, RELAYED[1] + RELAYED[2] + ALONG_X)
    others = row_router.at[:, pl.ds(0, (shards - 1) * width)]
    local(others, rt1_recv).wait()

    @pl.loop(1, experts)
    def _(k):
        pltpu.make_async_remote_copy(
            src_ref=row_router, dst_ref=all_router.at[mine], send_sem=rt2_send, recv_sem=rt2_recv,
            device_id={"expert": lax.rem(mine + k, experts)}, device_id_type=MESH,
        ).start()

    all_router[mine] = row_router[...]

    forward_groups(0, 0, 3)
    late = range(len(chunks) - 1, 0, -1)
    for c in late:
        send_pieces(c, RELAYED[0] + ALONG_Y + RELAYED[1] + RELAYED[2])

    for c in late[:-1]:
        forward_groups(c, 0, 3)
    forward_groups(late[-1], 0, 2)
    for c in late:
        send_pieces(c, ALONG_X)
    forward_groups(late[-1], 2, 3)

    def keep(e, tall, value):
        final[e, tall, columns] = value

    for c in range(len(chunks)):
        scaled(0, c, keep)

    root = jnp.sqrt(jnp.where(lane < SLOT, of_owner(first_total, me), rest_total[...]))
    for e in range(held):
        for c in range(0, rows, LANES):
            size = min(LANES, rows - c)
            spread = jnp.zeros((8, LANES), jnp.float32)
            for g in range(c // 8, (c + size) // 8):
                at = e * HALF + g
                spread = jnp.where(lane // 8 == g - c // 8, jnp.broadcast_to(root[:, at : at + 1], (8, LANES)), spread)
            line = jnp.sum(jnp.where(sublane == lane % 8, spread, 0.0), axis=0, keepdims=True)
            scale[e : e + 1, c : c + size] = line[:, :size]

    local(all_router.at[pl.ds(0, experts - 1)], rt2_recv).wait()
    router[...] = all_router[...].reshape(router.shape)

    local(first_got.at[pl.ds(0, shards - 1)], first_send).wait()
    local(part.at[pl.ds(1, shards - 1)], part_send).wait()
    local(got.at[pl.ds(1, shards - 1)], inv_send).wait()
    local(others, rt1_send).wait()
    local(all_router.at[pl.ds(0, experts - 1)], rt2_send).wait()
    local(ready.at[pl.ds(1, shards - 1)], row_send).wait()
    local(ready.at[pl.ds(0, (SIDE - 1) * (SIDE - 1))], forward_send).wait()
    local(ready.at[pl.ds(1, shards - 1)], row_recv).wait()


def hand_out_kernel(final, scale, router, final_out, scale_out, router_out, sem):
    copies = [(scale, scale_out), (router, router_out)]
    held, rows, _ = final.shape
    for e in range(held):
        for start in range(0, rows, PIECE):
            at = (e, pl.ds(start, min(PIECE, rows - start)))
            copies.append((final.at[at], final_out.at[at]))
    copies = [pltpu.make_async_copy(source, target, sem.at[n]) for n, (source, target) in enumerate(copies)]
    for copy in copies:
        copy.start()
    for copy in copies:
        copy.wait()


def hand_out(*arrays):
    held, rows, _ = arrays[0].shape
    return pl.pallas_call(
        hand_out_kernel,
        name="hand_out",
        out_shape=tuple(jax.ShapeDtypeStruct(x.shape, x.dtype) for x in arrays),
        in_specs=[pl.BlockSpec(memory_space=pltpu.VMEM)] * 3,
        out_specs=(pl.BlockSpec(memory_space=pltpu.HBM),) * 3,
        scratch_shapes=[pltpu.SemaphoreType.DMA((2 + held * pl.cdiv(rows, PIECE),))],
        compiler_params=pltpu.CompilerParams(vmem_limit_bytes=8 * 1024 * 1024),
    )(*arrays)


def solution(mesh):
    shards, experts = mesh.shape["shard"], mesh.shape["expert"]

    def local(master, second, weight, gain):
        held, length, width = master.shape
        rows = length // shards
        dma = pltpu.SemaphoreType.DMA
        wide = (shards, held, rows, width)
        final, scale, router = pl.pallas_call(
            functools.partial(kernel, shards, experts),
            name="serve",
            out_shape=(
                jax.ShapeDtypeStruct((held, rows, width * shards), jnp.bfloat16),
                jax.ShapeDtypeStruct((held, rows), jnp.float32),
                jax.ShapeDtypeStruct((experts * held, width * shards), jnp.bfloat16),
            ),
            in_specs=[pl.BlockSpec(memory_space=pltpu.HBM)] * 4,
            out_specs=(pl.BlockSpec(memory_space=pltpu.VMEM),) * 3,
            scratch_shapes=[
                pltpu.VMEM(wide, jnp.float32),
                pltpu.VMEM(wide, jnp.bfloat16),
                pltpu.VMEM(wide, jnp.bfloat16),
                pltpu.VMEM(wide, jnp.bfloat16),
                pltpu.VMEM((shards, 2, 8, LANES), jnp.float32),
                pltpu.VMEM((2, 8, LANES), jnp.float32),
                pltpu.VMEM((2, 8, LANES), jnp.float32),
                pltpu.VMEM((shards, 8, LANES), jnp.float32),
                pltpu.VMEM((shards, 8, LANES), jnp.float32),
                pltpu.VMEM((8, LANES), jnp.float32),
                pltpu.VMEM((shards, 8, LANES), jnp.float32),
                pltpu.VMEM((held, width), jnp.bfloat16),
                pltpu.VMEM((held, width * shards), jnp.bfloat16),
                pltpu.VMEM((experts, held, width * shards), jnp.bfloat16),
                pltpu.VMEM((held, width), jnp.float32),
                pltpu.VMEM((1, width), jnp.float32),
                dma, dma((shards,)), dma, dma, dma, dma, dma, dma, dma, dma((shards,)),
                dma, dma, dma, dma, dma(((held + 1) * SIDE,)), dma, dma, dma,
            ],
            compiler_params=pltpu.CompilerParams(
                collective_id=0, has_side_effects=True, vmem_limit_bytes=44 * 1024 * 1024
            ),
        )(*[pltpu.with_memory_space_constraint(x, pltpu.HBM) for x in (master, second, weight.T, gain[None, :])])
        final, scale, router = hand_out(final, scale, router)
        return final, scale, router.T

    return jax.shard_map(
        local,
        mesh=mesh,
        in_specs=(P("expert", None, "shard"), P("expert", None, "shard"), P("shard", "expert"), P("shard")),
        out_specs=(P("expert", "shard", None), P("expert", "shard"), P()),
        check_vma=False,
    )
```

```python
import functools

import jax
import jax.numpy as jnp
from jax import lax
from jax.experimental import pallas as pl
from jax.experimental.pallas import tpu as pltpu
from jax.sharding import PartitionSpec as P

MESH = pl.DeviceIdType.MESH
SIDE = 4
LANES = 128
HALF = LANES // 2
PIECE = 80

RELAYED = ((5, 15, 10), (7, 14, 9), (11, 6, 13))
Y_FIRST = ((1,), (1,), (1,))
ALONG_X = (2, 1, 3)
ALONG_Y = (4, 12, 8)
GROUP = tuple(next((n for n, group in enumerate(RELAYED) if k in group), 0) for k in range(SIDE * SIDE))
FIRST = 128
SLOT = FIRST // 8


def pick(table, i):
    value = jnp.int32(table[0])
    for n, entry in enumerate(table[1:], 1):
        value = jnp.where(i == n, jnp.int32(entry), value)
    return value


def toward(shard, k):
    y, x = lax.div(shard, SIDE), lax.rem(shard, SIDE)
    return lax.rem(y + lax.div(k, SIDE), SIDE) * SIDE + lax.rem(x + lax.rem(k, SIDE), SIDE)


def away(shard, k):
    y, x = lax.div(shard, SIDE), lax.rem(shard, SIDE)
    return lax.rem(y + SIDE - lax.div(k, SIDE), SIDE) * SIDE + lax.rem(x + SIDE - lax.rem(k, SIDE), SIDE)


def kernel(
    shards, experts,
    master, second, weight_in, gain_in,
    final, scale, router,
    wide, narrow, ready, stage, first_got, first_total, first_inverse, part, got, rest_total, inverse,
    one_router, row_router, all_router, weight, gain,
    first_read, rest_read, weight_read, gain_read, first_send, first_recv, part_send, part_recv, inv_send, inv_recv,
    rt1_send, rt1_recv, rt2_send, rt2_recv, relay_recv, row_send, forward_send, row_recv,
):
    me = lax.axis_index("shard")
    mine = lax.axis_index("expert")
    held, rows, width = wide.shape[1:]
    columns = pl.ds(pl.multiple_of(me * width, LANES), width)
    chunks = ((0, 0, FIRST), (0, FIRST, rows - FIRST)) + tuple((e, 0, rows) for e in range(1, held))

    def local(ref, sem):
        return pltpu.make_async_copy(ref, ref, sem)

    def read(k, c, sem):
        e, start, count = chunks[c]
        source = pl.ds(pl.multiple_of(toward(me, k) * rows + start, 16), count)
        target = pl.ds(start, count)
        pltpu.make_async_copy(master.at[e, source], wide.at[k, e, target], sem).start()
        pltpu.make_async_copy(second.at[e, source], narrow.at[k, e, target], sem).start()

    read_weight = pltpu.make_async_copy(weight_in, weight, weight_read)
    read_gain = pltpu.make_async_copy(gain_in, gain, gain_read)
    read_weight.start()
    read_gain.start()

    barrier = pltpu.get_barrier_semaphore()

    @pl.loop(1, shards, unroll=True)
    def _(k):
        pl.semaphore_signal(barrier, inc=1, device_id={"shard": toward(me, k)}, device_id_type=MESH)

    @pl.loop(1, experts, unroll=True)
    def _(k):
        pl.semaphore_signal(barrier, inc=1, device_id={"expert": lax.rem(mine + k, experts)}, device_id_type=MESH)

    @pl.loop(0, shards)
    def _(k):
        read(k, 0, first_read)

    @pl.loop(1, shards + 1)
    def _(k):
        for c in range(1, len(chunks)):
            read(lax.rem(k, shards), c, rest_read.at[lax.rem(k, shards)])

    lane = lax.broadcasted_iota(jnp.int32, (8, LANES), 1)
    sublane = lax.broadcasted_iota(jnp.int32, (8, LANES), 0)

    def sums_of(k, c, packed, base):
        e, start, count = chunks[c]
        for g in range(start // 8, (start + count) // 8, 2):
            tall = pl.ds(8 * g, 16)
            merged = wide[k, e, tall, :] + narrow[k, e, tall, :].astype(jnp.float32)
            sums = jnp.sum(merged * merged, axis=1, keepdims=True)
            for h in range(2):
                packed = jnp.where(lane == base + g + h, sums[8 * h : 8 * h + 8], packed)
        return packed

    local(narrow.at[:, 0, pl.ds(0, 3 * FIRST)], first_read).wait()

    def first_sums(i, packed):
        for k in [4 * i + n for n in range(4)]:
            owner = toward(me, k)
            base = lax.rem(owner, 8) * SLOT
            low = owner < 8
            sums = sums_of(k, 0, zero, base)
            packed = packed[0] + jnp.where(low, sums, 0.0), packed[1] + jnp.where(low, 0.0, sums)
        return packed

    zero = jnp.zeros((8, LANES), jnp.float32)
    packed = lax.fori_loop(0, shards // 4, first_sums, (zero, zero))
    first_got[me, 0] = packed[0]
    first_got[me, 1] = packed[1]
    pl.semaphore_wait(barrier, shards + experts - 2)

    @pl.loop(1, shards, unroll=True)
    def _(k):
        pltpu.make_async_remote_copy(
            src_ref=first_got.at[me], dst_ref=first_got.at[me], send_sem=first_send, recv_sem=first_recv,
            device_id={"shard": toward(me, k)}, device_id_type=MESH,
        ).start()

    read_weight.wait()
    read_gain.wait()
    mine_router = (weight[...] * gain[...]).astype(jnp.bfloat16)
    one_router[...] = mine_router
    row_router[:, columns] = mine_router

    @pl.loop(1, shards)
    def _(k):
        pltpu.make_async_remote_copy(
            src_ref=one_router, dst_ref=row_router.at[:, columns], send_sem=rt1_send, recv_sem=rt1_recv,
            device_id={"shard": toward(me, k)}, device_id_type=MESH,
        ).start()

    def rest_sums(k):
        local(narrow.at[pl.ds(0, 3), :, pl.ds(0, (held * rows - FIRST) // held)], rest_read.at[k]).wait()
        packed = zero
        for c in range(1, len(chunks)):
            packed = sums_of(k, c, packed, chunks[c][0] * HALF)
        part[k] = packed

    @pl.loop(1, shards)
    def _(k):
        rest_sums(k)
        pltpu.make_async_remote_copy(
            src_ref=part.at[k], dst_ref=got.at[k], send_sem=part_send, recv_sem=part_recv,
            device_id={"shard": toward(me, k)}, device_id_type=MESH,
        ).start()

    rest_sums(0)

    local(first_got.at[pl.ds(0, shards - 1)], first_recv).wait()
    for v in range(2):
        total = first_got[0, v]
        for d in range(1, shards):
            total += first_got[d, v]
        first_total[v] = total
        first_inverse[v] = 1.0 / jnp.sqrt(total)

    def of_owner(ref, owner):
        return pltpu.roll(ref[lax.div(owner, 8)], lax.rem(LANES - lax.rem(owner, 8) * SLOT, LANES), 1)

    def scaled(k, c, store):
        e, start, count = chunks[c]
        factors = of_owner(first_inverse, toward(me, k)) if c == 0 else inverse[k]
        for g in range(start // 8, (start + count) // 8, 2):
            tall = pl.ds(8 * g, 16)
            merged = wide[k, e, tall, :] + narrow[k, e, tall, :].astype(jnp.float32)
            at = [e * HALF + g + h for h in range(2)]
            factor = jnp.concatenate([jnp.broadcast_to(factors[:, a : a + 1], (8, width)) for a in at], axis=0)
            store(e, tall, (merged * factor).astype(jnp.bfloat16))

    def first_hop(c, k):
        swapped = sum([RELAYED[n] for n in Y_FIRST[c]], ())
        return pick([n - n % SIDE if n in swapped else n % SIDE for n in range(shards)], k)

    def send_pieces(c, offsets):
        e, start, count = chunks[c]
        part_rows = pl.ds(start, count)

        @pl.loop(0, len(offsets))
        def _(i):
            k = pick(offsets, i)
            dy, dx = lax.div(k, SIDE), lax.rem(k, SIDE)

            if c == held:
                local(inverse.at[k], inv_recv.at[k]).wait()

            def store(e, tall, value):
                ready[k, e, tall, :] = value

            scaled(k, c, store)

            @pl.when((dy != 0) & (dx != 0))
            def _():
                pltpu.make_async_remote_copy(
                    src_ref=ready.at[k, e, part_rows], dst_ref=stage.at[k, e, part_rows],
                    send_sem=row_send, recv_sem=relay_recv.at[c * SIDE + pick(GROUP, k)],
                    device_id={"shard": toward(me, first_hop(c, k))}, device_id_type=MESH,
                ).start()

            @pl.when((dy == 0) | (dx == 0))
            def _():
                pltpu.make_async_remote_copy(
                    src_ref=ready.at[k, e, part_rows], dst_ref=final.at[e, part_rows, columns],
                    send_sem=row_send, recv_sem=row_recv,
                    device_id={"shard": toward(me, k)}, device_id_type=MESH,
                ).start()

    def forward_groups(c, begin, end):
        e, start, count = chunks[c]
        part_rows = pl.ds(start, count)

        @pl.loop(begin, end)
        def _(i):
            local(stage.at[pl.ds(0, SIDE - 1), e, part_rows], relay_recv.at[c * SIDE + i]).wait()

            @pl.loop(0, SIDE - 1)
            def _(j):
                k = pick(sum(RELAYED, ()), i * (SIDE - 1) + j)
                hop = first_hop(c, k)
                origin = pl.ds(pl.multiple_of(away(me, hop) * width, LANES), width)
                pltpu.make_async_remote_copy(
                    src_ref=stage.at[k, e, part_rows], dst_ref=final.at[e, part_rows, origin],
                    send_sem=forward_send, recv_sem=row_recv,
                    device_id={"shard": toward(me, k - hop)}, device_id_type=MESH,
                ).start()

    send_pieces(0, RELAYED[0] + ALONG_Y)

    local(got.at[pl.ds(1, shards - 1)], part_recv).wait()
    total = part[0]
    for k in range(1, shards):
        total += got[k]
    rest_total[...] = total
    inverse[0] = 1.0 / jnp.sqrt(total)

    @pl.loop(1, shards)
    def _(k):
        pltpu.make_async_remote_copy(
            src_ref=inverse.at[0], dst_ref=inverse.at[k], send_sem=inv_send, recv_sem=inv_recv.at[k],
            device_id={"shard": away(me, k)}, device_id_type=MESH,
        ).start()

    send_pieces(0, RELAYED[1] + RELAYED[2] + ALONG_X)
    others = row_router.at[:, pl.ds(0, (shards - 1) * width)]
    local(others, rt1_recv).wait()

    @pl.loop(1, experts)
    def _(k):
        pltpu.make_async_remote_copy(
            src_ref=row_router, dst_ref=all_router.at[mine], send_sem=rt2_send, recv_sem=rt2_recv,
            device_id={"expert": lax.rem(mine + k, experts)}, device_id_type=MESH,
        ).start()

    all_router[mine] = row_router[...]

    forward_groups(0, 0, 3)
    late = range(len(chunks) - 1, 0, -1)
    for c in late:
        send_pieces(c, RELAYED[0] + ALONG_Y + RELAYED[1] + RELAYED[2])

    for c in late[:-1]:
        forward_groups(c, 0, 3)
    forward_groups(late[-1], 0, 2)
    for c in late:
        send_pieces(c, ALONG_X)
    forward_groups(late[-1], 2, 3)

    def keep(e, tall, value):
        final[e, tall, columns] = value

    for c in range(len(chunks)):
        scaled(0, c, keep)

    root = jnp.sqrt(jnp.where(lane < SLOT, of_owner(first_total, me), rest_total[...]))
    for e in range(held):
        for c in range(0, rows, LANES):
            size = min(LANES, rows - c)
            spread = jnp.zeros((8, LANES), jnp.float32)
            for g in range(c // 8, (c + size) // 8):
                at = e * HALF + g
                spread = jnp.where(lane // 8 == g - c // 8, jnp.broadcast_to(root[:, at : at + 1], (8, LANES)), spread)
            line = jnp.sum(jnp.where(sublane == lane % 8, spread, 0.0), axis=0, keepdims=True)
            scale[e : e + 1, c : c + size] = line[:, :size]

    local(all_router.at[pl.ds(0, experts - 1)], rt2_recv).wait()
    router[...] = all_router[...].reshape(router.shape)

    local(first_got.at[pl.ds(0, shards - 1)], first_send).wait()
    local(part.at[pl.ds(1, shards - 1)], part_send).wait()
    local(got.at[pl.ds(1, shards - 1)], inv_send).wait()
    local(others, rt1_send).wait()
    local(all_router.at[pl.ds(0, experts - 1)], rt2_send).wait()
    local(ready.at[pl.ds(1, shards - 1)], row_send).wait()
    local(ready.at[pl.ds(0, (SIDE - 1) * (SIDE - 1))], forward_send).wait()
    local(ready.at[pl.ds(1, shards - 1)], row_recv).wait()


def hand_out_kernel(final, scale, router, final_out, scale_out, router_out, sem):
    copies = [(scale, scale_out), (router, router_out)]
    held, rows, _ = final.shape
    for e in range(held):
        for start in range(0, rows, PIECE):
            at = (e, pl.ds(start, min(PIECE, rows - start)))
            copies.append((final.at[at], final_out.at[at]))
    copies = [pltpu.make_async_copy(source, target, sem.at[n]) for n, (source, target) in enumerate(copies)]
    for copy in copies:
        copy.start()
    for copy in copies:
        copy.wait()


def hand_out(*arrays):
    held, rows, _ = arrays[0].shape
    return pl.pallas_call(
        hand_out_kernel,
        name="hand_out",
        out_shape=tuple(jax.ShapeDtypeStruct(x.shape, x.dtype) for x in arrays),
        in_specs=[pl.BlockSpec(memory_space=pltpu.VMEM)] * 3,
        out_specs=(pl.BlockSpec(memory_space=pltpu.HBM),) * 3,
        scratch_shapes=[pltpu.SemaphoreType.DMA((2 + held * pl.cdiv(rows, PIECE),))],
        compiler_params=pltpu.CompilerParams(vmem_limit_bytes=8 * 1024 * 1024),
    )(*arrays)


def solution(mesh):
    shards, experts = mesh.shape["shard"], mesh.shape["expert"]

    def local(master, second, weight, gain):
        held, length, width = master.shape
        rows = length // shards
        dma = pltpu.SemaphoreType.DMA
        wide = (shards, held, rows, width)
        final, scale, router = pl.pallas_call(
            functools.partial(kernel, shards, experts),
            name="serve",
            out_shape=(
                jax.ShapeDtypeStruct((held, rows, width * shards), jnp.bfloat16),
                jax.ShapeDtypeStruct((held, rows), jnp.float32),
                jax.ShapeDtypeStruct((experts * held, width * shards), jnp.bfloat16),
            ),
            in_specs=[pl.BlockSpec(memory_space=pltpu.HBM)] * 4,
            out_specs=(pl.BlockSpec(memory_space=pltpu.VMEM),) * 3,
            scratch_shapes=[
                pltpu.VMEM(wide, jnp.float32),
                pltpu.VMEM(wide, jnp.bfloat16),
                pltpu.VMEM(wide, jnp.bfloat16),
                pltpu.VMEM(wide, jnp.bfloat16),
                pltpu.VMEM((shards, 2, 8, LANES), jnp.float32),
                pltpu.VMEM((2, 8, LANES), jnp.float32),
                pltpu.VMEM((2, 8, LANES), jnp.float32),
                pltpu.VMEM((shards, 8, LANES), jnp.float32),
                pltpu.VMEM((shards, 8, LANES), jnp.float32),
                pltpu.VMEM((8, LANES), jnp.float32),
                pltpu.VMEM((shards, 8, LANES), jnp.float32),
                pltpu.VMEM((held, width), jnp.bfloat16),
                pltpu.VMEM((held, width * shards), jnp.bfloat16),
                pltpu.VMEM((experts, held, width * shards), jnp.bfloat16),
                pltpu.VMEM((held, width), jnp.float32),
                pltpu.VMEM((1, width), jnp.float32),
                dma, dma((shards,)), dma, dma, dma, dma, dma, dma, dma, dma((shards,)),
                dma, dma, dma, dma, dma(((held + 1) * SIDE,)), dma, dma, dma,
            ],
            compiler_params=pltpu.CompilerParams(
                collective_id=0, has_side_effects=True, vmem_limit_bytes=44 * 1024 * 1024
            ),
        )(*[pltpu.with_memory_space_constraint(x, pltpu.HBM) for x in (master, second, weight.T, gain[None, :])])
        final, scale, router = hand_out(final, scale, router)
        return final, scale, router.T

    return jax.shard_map(
        local,
        mesh=mesh,
        in_specs=(P("expert", None, "shard"), P("expert", None, "shard"), P("shard", "expert"), P("shard")),
        out_specs=(P("expert", "shard", None), P("expert", "shard"), P()),
        check_vma=False,
    )
```

```python
import functools

import jax
import jax.numpy as jnp
from jax import lax
from jax.experimental import pallas as pl
from jax.experimental.pallas import tpu as pltpu
from jax.sharding import PartitionSpec as P

MESH = pl.DeviceIdType.MESH
SIDE = 4
LANES = 128
HALF = LANES // 2
PIECE = 80

RELAYED = ((5, 15, 10), (7, 14, 9), (11, 6, 13))
Y_FIRST = ((1,), (1,), (1,))
ALONG_X = (2, 1, 3)
ALONG_Y = (4, 12, 8)
GROUP = tuple(next((n for n, group in enumerate(RELAYED) if k in group), 0) for k in range(SIDE * SIDE))
FIRST = 128
SLOT = FIRST // 8


def pick(table, i):
    value = jnp.int32(table[0])
    for n, entry in enumerate(table[1:], 1):
        value = jnp.where(i == n, jnp.int32(entry), value)
    return value


def toward(shard, k):
    y, x = lax.div(shard, SIDE), lax.rem(shard, SIDE)
    return lax.rem(y + lax.div(k, SIDE), SIDE) * SIDE + lax.rem(x + lax.rem(k, SIDE), SIDE)


def away(shard, k):
    y, x = lax.div(shard, SIDE), lax.rem(shard, SIDE)
    return lax.rem(y + SIDE - lax.div(k, SIDE), SIDE) * SIDE + lax.rem(x + SIDE - lax.rem(k, SIDE), SIDE)


def kernel(
    shards, experts,
    master, second, weight_in, gain_in,
    final, scale, router,
    wide, narrow, ready, stage, first_got, first_total, first_inverse, part, got, rest_total, inverse,
    one_router, row_router, all_router, weight, gain,
    first_read, rest_read, weight_read, gain_read, first_send, first_recv, part_send, part_recv, inv_send, inv_recv,
    rt1_send, rt1_recv, rt2_send, rt2_recv, relay_recv, row_send, forward_send, row_recv,
):
    me = lax.axis_index("shard")
    mine = lax.axis_index("expert")
    held, rows, width = wide.shape[1:]
    columns = pl.ds(pl.multiple_of(me * width, LANES), width)
    chunks = ((0, 0, FIRST), (0, FIRST, rows - FIRST)) + tuple((e, 0, rows) for e in range(1, held))

    def local(ref, sem):
        return pltpu.make_async_copy(ref, ref, sem)

    def read(k, c, sem):
        e, start, count = chunks[c]
        source = pl.ds(pl.multiple_of(toward(me, k) * rows + start, 16), count)
        target = pl.ds(start, count)
        pltpu.make_async_copy(master.at[e, source], wide.at[k, e, target], sem).start()
        pltpu.make_async_copy(second.at[e, source], narrow.at[k, e, target], sem).start()

    read_weight = pltpu.make_async_copy(weight_in, weight, weight_read)
    read_gain = pltpu.make_async_copy(gain_in, gain, gain_read)
    read_weight.start()
    read_gain.start()

    barrier = pltpu.get_barrier_semaphore()

    @pl.loop(1, shards, unroll=True)
    def _(k):
        pl.semaphore_signal(barrier, inc=1, device_id={"shard": toward(me, k)}, device_id_type=MESH)

    @pl.loop(1, experts, unroll=True)
    def _(k):
        pl.semaphore_signal(barrier, inc=1, device_id={"expert": lax.rem(mine + k, experts)}, device_id_type=MESH)

    @pl.loop(0, shards)
    def _(k):
        read(k, 0, first_read)

    @pl.loop(1, shards + 1)
    def _(k):
        for c in range(1, len(chunks)):
            read(lax.rem(k, shards), c, rest_read.at[lax.rem(k, shards)])

    lane = lax.broadcasted_iota(jnp.int32, (8, LANES), 1)
    sublane = lax.broadcasted_iota(jnp.int32, (8, LANES), 0)

    def sums_of(k, c, packed, base):
        e, start, count = chunks[c]
        for g in range(start // 8, (start + count) // 8, 2):
            tall = pl.ds(8 * g, 16)
            merged = wide[k, e, tall, :] + narrow[k, e, tall, :].astype(jnp.float32)
            sums = jnp.sum(merged * merged, axis=1, keepdims=True)
            for h in range(2):
                packed = jnp.where(lane == base + g + h, sums[8 * h : 8 * h + 8], packed)
        return packed

    local(narrow.at[:, 0, pl.ds(0, 3 * FIRST)], first_read).wait()

    def first_sums(i, packed):
        for k in [4 * i + n for n in range(4)]:
            owner = toward(me, k)
            base = lax.rem(owner, 8) * SLOT
            low = owner < 8
            sums = sums_of(k, 0, zero, base)
            packed = packed[0] + jnp.where(low, sums, 0.0), packed[1] + jnp.where(low, 0.0, sums)
        return packed

    zero = jnp.zeros((8, LANES), jnp.float32)
    packed = lax.fori_loop(0, shards // 4, first_sums, (zero, zero))
    first_got[me, 0] = packed[0]
    first_got[me, 1] = packed[1]
    pl.semaphore_wait(barrier, shards + experts - 2)

    @pl.loop(1, shards, unroll=True)
    def _(k):
        pltpu.make_async_remote_copy(
            src_ref=first_got.at[me], dst_ref=first_got.at[me], send_sem=first_send, recv_sem=first_recv,
            device_id={"shard": toward(me, k)}, device_id_type=MESH,
        ).start()

    read_weight.wait()
    read_gain.wait()
    mine_router = (weight[...] * gain[...]).astype(jnp.bfloat16)
    one_router[...] = mine_router
    row_router[:, columns] = mine_router

    @pl.loop(1, shards)
    def _(k):
        pltpu.make_async_remote_copy(
            src_ref=one_router, dst_ref=row_router.at[:, columns], send_sem=rt1_send, recv_sem=rt1_recv,
            device_id={"shard": toward(me, k)}, device_id_type=MESH,
        ).start()

    def rest_sums(k):
        local(narrow.at[pl.ds(0, 3), :, pl.ds(0, (held * rows - FIRST) // held)], rest_read.at[k]).wait()
        packed = zero
        for c in range(1, len(chunks)):
            packed = sums_of(k, c, packed, chunks[c][0] * HALF)
        part[k] = packed

    @pl.loop(1, shards)
    def _(k):
        rest_sums(k)
        pltpu.make_async_remote_copy(
            src_ref=part.at[k], dst_ref=got.at[k], send_sem=part_send, recv_sem=part_recv,
            device_id={"shard": toward(me, k)}, device_id_type=MESH,
        ).start()

    rest_sums(0)

    local(first_got.at[pl.ds(0, shards - 1)], first_recv).wait()
    for v in range(2):
        total = first_got[0, v]
        for d in range(1, shards):
            total += first_got[d, v]
        first_total[v] = total
        first_inverse[v] = 1.0 / jnp.sqrt(total)

    def of_owner(ref, owner):
        return pltpu.roll(ref[lax.div(owner, 8)], lax.rem(LANES - lax.rem(owner, 8) * SLOT, LANES), 1)

    def scaled(k, c, store):
        e, start, count = chunks[c]
        factors = of_owner(first_inverse, toward(me, k)) if c == 0 else inverse[k]
        for g in range(start // 8, (start + count) // 8, 2):
            tall = pl.ds(8 * g, 16)
            merged = wide[k, e, tall, :] + narrow[k, e, tall, :].astype(jnp.float32)
            at = [e * HALF + g + h for h in range(2)]
            factor = jnp.concatenate([jnp.broadcast_to(factors[:, a : a + 1], (8, width)) for a in at], axis=0)
            store(e, tall, (merged * factor).astype(jnp.bfloat16))

    def first_hop(c, k):
        swapped = sum([RELAYED[n] for n in Y_FIRST[c]], ())
        return pick([n - n % SIDE if n in swapped else n % SIDE for n in range(shards)], k)

    def send_pieces(c, offsets):
        e, start, count = chunks[c]
        part_rows = pl.ds(start, count)

        @pl.loop(0, len(offsets))
        def _(i):
            k = pick(offsets, i)
            dy, dx = lax.div(k, SIDE), lax.rem(k, SIDE)

            def store(e, tall, value):
                ready[k, e, tall, :] = value

            scaled(k, c, store)

            @pl.when((dy != 0) & (dx != 0))
            def _():
                pltpu.make_async_remote_copy(
                    src_ref=ready.at[k, e, part_rows], dst_ref=stage.at[k, e, part_rows],
                    send_sem=row_send, recv_sem=relay_recv.at[c * SIDE + pick(GROUP, k)],
                    device_id={"shard": toward(me, first_hop(c, k))}, device_id_type=MESH,
                ).start()

            @pl.when((dy == 0) | (dx == 0))
            def _():
                pltpu.make_async_remote_copy(
                    src_ref=ready.at[k, e, part_rows], dst_ref=final.at[e, part_rows, columns],
                    send_sem=row_send, recv_sem=row_recv,
                    device_id={"shard": toward(me, k)}, device_id_type=MESH,
                ).start()

    def forward_groups(c, begin, end):
        e, start, count = chunks[c]
        part_rows = pl.ds(start, count)

        @pl.loop(begin, end)
        def _(i):
            local(stage.at[pl.ds(0, SIDE - 1), e, part_rows], relay_recv.at[c * SIDE + i]).wait()

            @pl.loop(0, SIDE - 1)
            def _(j):
                k = pick(sum(RELAYED, ()), i * (SIDE - 1) + j)
                hop = first_hop(c, k)
                origin = pl.ds(pl.multiple_of(away(me, hop) * width, LANES), width)
                pltpu.make_async_remote_copy(
                    src_ref=stage.at[k, e, part_rows], dst_ref=final.at[e, part_rows, origin],
                    send_sem=forward_send, recv_sem=row_recv,
                    device_id={"shard": toward(me, k - hop)}, device_id_type=MESH,
                ).start()

    send_pieces(0, RELAYED[0] + ALONG_Y)

    local(got.at[pl.ds(1, shards - 1)], part_recv).wait()
    total = part[0]
    for k in range(1, shards):
        total += got[k]
    rest_total[...] = total
    inverse[0] = 1.0 / jnp.sqrt(total)

    @pl.loop(1, shards)
    def _(k):
        pltpu.make_async_remote_copy(
            src_ref=inverse.at[0], dst_ref=inverse.at[k], send_sem=inv_send, recv_sem=inv_recv,
            device_id={"shard": away(me, k)}, device_id_type=MESH,
        ).start()

    send_pieces(0, RELAYED[1] + RELAYED[2] + ALONG_X)
    others = row_router.at[:, pl.ds(0, (shards - 1) * width)]
    local(others, rt1_recv).wait()

    @pl.loop(1, experts)
    def _(k):
        pltpu.make_async_remote_copy(
            src_ref=row_router, dst_ref=all_router.at[mine], send_sem=rt2_send, recv_sem=rt2_recv,
            device_id={"expert": lax.rem(mine + k, experts)}, device_id_type=MESH,
        ).start()

    all_router[mine] = row_router[...]

    forward_groups(0, 0, 3)
    local(inverse.at[pl.ds(1, shards - 1)], inv_recv).wait()
    late = range(len(chunks) - 1, 0, -1)
    for c in late:
        send_pieces(c, RELAYED[0] + ALONG_Y + RELAYED[1] + RELAYED[2])

    for c in late[:-1]:
        forward_groups(c, 0, 3)
    forward_groups(late[-1], 0, 2)
    for c in late:
        send_pieces(c, ALONG_X)
    forward_groups(late[-1], 2, 3)

    def keep(e, tall, value):
        final[e, tall, columns] = value

    for c in range(len(chunks)):
        scaled(0, c, keep)

    root = jnp.sqrt(jnp.where(lane < SLOT, of_owner(first_total, me), rest_total[...]))
    for e in range(held):
        for c in range(0, rows, LANES):
            size = min(LANES, rows - c)
            spread = jnp.zeros((8, LANES), jnp.float32)
            for g in range(c // 8, (c + size) // 8):
                at = e * HALF + g
                spread = jnp.where(lane // 8 == g - c // 8, jnp.broadcast_to(root[:, at : at + 1], (8, LANES)), spread)
            line = jnp.sum(jnp.where(sublane == lane % 8, spread, 0.0), axis=0, keepdims=True)
            scale[e : e + 1, c : c + size] = line[:, :size]

    local(all_router.at[pl.ds(0, experts - 1)], rt2_recv).wait()
    router[...] = all_router[...].reshape(router.shape)

    local(first_got.at[pl.ds(0, shards - 1)], first_send).wait()
    local(part.at[pl.ds(1, shards - 1)], part_send).wait()
    local(got.at[pl.ds(1, shards - 1)], inv_send).wait()
    local(others, rt1_send).wait()
    local(all_router.at[pl.ds(0, experts - 1)], rt2_send).wait()
    local(ready.at[pl.ds(1, shards - 1)], row_send).wait()
    local(ready.at[pl.ds(0, (SIDE - 1) * (SIDE - 1))], forward_send).wait()
    local(ready.at[pl.ds(1, shards - 1)], row_recv).wait()


def hand_out_kernel(final, scale, router, final_out, scale_out, router_out, sem):
    copies = [(scale, scale_out), (router, router_out)]
    held, rows, _ = final.shape
    for e in range(held):
        for start in range(0, rows, PIECE):
            at = (e, pl.ds(start, min(PIECE, rows - start)))
            copies.append((final.at[at], final_out.at[at]))
    copies = [pltpu.make_async_copy(source, target, sem.at[n]) for n, (source, target) in enumerate(copies)]
    for copy in copies:
        copy.start()
    for copy in copies:
        copy.wait()


def hand_out(*arrays):
    held, rows, _ = arrays[0].shape
    return pl.pallas_call(
        hand_out_kernel,
        name="hand_out",
        out_shape=tuple(jax.ShapeDtypeStruct(x.shape, x.dtype) for x in arrays),
        in_specs=[pl.BlockSpec(memory_space=pltpu.VMEM)] * 3,
        out_specs=(pl.BlockSpec(memory_space=pltpu.HBM),) * 3,
        scratch_shapes=[pltpu.SemaphoreType.DMA((2 + held * pl.cdiv(rows, PIECE),))],
        compiler_params=pltpu.CompilerParams(vmem_limit_bytes=8 * 1024 * 1024),
    )(*arrays)


def solution(mesh):
    shards, experts = mesh.shape["shard"], mesh.shape["expert"]

    def local(master, second, weight, gain):
        held, length, width = master.shape
        rows = length // shards
        dma = pltpu.SemaphoreType.DMA
        wide = (shards, held, rows, width)
        final, scale, router = pl.pallas_call(
            functools.partial(kernel, shards, experts),
            name="serve",
            out_shape=(
                jax.ShapeDtypeStruct((held, rows, width * shards), jnp.bfloat16),
                jax.ShapeDtypeStruct((held, rows), jnp.float32),
                jax.ShapeDtypeStruct((experts * held, width * shards), jnp.bfloat16),
            ),
            in_specs=[pl.BlockSpec(memory_space=pltpu.HBM)] * 4,
            out_specs=(pl.BlockSpec(memory_space=pltpu.VMEM),) * 3,
            scratch_shapes=[
                pltpu.VMEM(wide, jnp.float32),
                pltpu.VMEM(wide, jnp.bfloat16),
                pltpu.VMEM(wide, jnp.bfloat16),
                pltpu.VMEM(wide, jnp.bfloat16),
                pltpu.VMEM((shards, 2, 8, LANES), jnp.float32),
                pltpu.VMEM((2, 8, LANES), jnp.float32),
                pltpu.VMEM((2, 8, LANES), jnp.float32),
                pltpu.VMEM((shards, 8, LANES), jnp.float32),
                pltpu.VMEM((shards, 8, LANES), jnp.float32),
                pltpu.VMEM((8, LANES), jnp.float32),
                pltpu.VMEM((shards, 8, LANES), jnp.float32),
                pltpu.VMEM((held, width), jnp.bfloat16),
                pltpu.VMEM((held, width * shards), jnp.bfloat16),
                pltpu.VMEM((experts, held, width * shards), jnp.bfloat16),
                pltpu.VMEM((held, width), jnp.float32),
                pltpu.VMEM((1, width), jnp.float32),
                dma, dma((shards,)), dma, dma, dma, dma, dma, dma, dma, dma,
                dma, dma, dma, dma, dma(((held + 1) * SIDE,)), dma, dma, dma,
            ],
            compiler_params=pltpu.CompilerParams(
                collective_id=0, has_side_effects=True, vmem_limit_bytes=44 * 1024 * 1024
            ),
        )(*[pltpu.with_memory_space_constraint(x, pltpu.HBM) for x in (master, second, weight.T, gain[None, :])])
        final, scale, router = hand_out(final, scale, router)
        return final, scale, router.T

    return jax.shard_map(
        local,
        mesh=mesh,
        in_specs=(P("expert", None, "shard"), P("expert", None, "shard"), P("shard", "expert"), P("shard")),
        out_specs=(P("expert", "shard", None), P("expert", "shard"), P()),
        check_vma=False,
    )
```
